32 devices in a mesh: rep: 1 (over z), dp: 32 (over x, y, core).
Axes of the slice: x: 4, y: 4, z: 1, core: 2. Of those that a mesh axis runs over, the one named last changes fastest.
The devices are a block of a 4x4x8 slice.
Arguments:
- x: bfloat16 [32, 2048, 1024], P(('rep', 'dp'))
- dy: bfloat16 [32, 2048, 1024], P(('rep', 'dp'))
- w_gate: bfloat16 [2, 1024, 2816], replicated
- w_up: bfloat16 [2, 1024, 2816], replicated
- w_down: bfloat16 [2, 2816, 1024], replicated
- m_w_gate: float32 [2, 1024, 2816], P(None, 'dp')
- m_w_up: float32 [2, 1024, 2816], P(None, 'dp')
- m_w_down: float32 [2, 2816, 1024], P(None, 'dp')
- v_w_gate: float32 [2, 1024, 2816], P(None, 'dp')
- v_w_up: float32 [2, 1024, 2816], P(None, 'dp')
- v_w_down: float32 [2, 2816, 1024], P(None, 'dp')
Outputs:
- output 1: bfloat16 [2, 1024, 2816], P('rep')
- output 2: bfloat16 [2, 1024, 2816], P('rep')
- output 3: bfloat16 [2, 2816, 1024], P('rep')
- output 4: float32 [2, 1024, 2816], P('rep', 'dp')
- output 5: float32 [2, 1024, 2816], P('rep', 'dp')
- output 6: float32 [2, 2816, 1024], P('rep', 'dp')
- output 7: float32 [2, 1024, 2816], P('rep', 'dp')
- output 8: float32 [2, 1024, 2816], P('rep', 'dp')
- output 9: float32 [2, 2816, 1024], P('rep', 'dp')
All inputs are finite; a program needn't handle non-finite values.
Results may differ from the reference program's by a relative error of at most 0.02.
Values are sent between devices in bfloat16 or wider.
A program may use at most 768 MiB of HBM per device.

```python
import jax
import jax.numpy as jnp
from jax import lax

SEQUENCES = 32
TOKENS = 2048
D = 1024
FF = 2816
LAYERS = 2
NAMES = ("w_gate", "w_up", "w_down")
SHAPES = {"w_gate": (LAYERS, D, FF), "w_up": (LAYERS, D, FF), "w_down": (LAYERS, FF, D)}


def bump(key, n, height):
    away = (jnp.arange(n, dtype=jnp.int32) - jax.random.randint(key, (), 0, n, jnp.int32)) % n
    return jnp.where(away < n // 8, height, 1.0)


def together(key, own, strength):
    shared = jax.random.normal(key, own.shape[1:], jnp.float32)
    return (own + strength * shared) * lax.rsqrt(1 + strength * strength)


def setup_inputs(seed: int = 0, part: int = 0) -> dict:
    kx, kdy, ka, kb, kz, kf, kh, kl, *keys = jax.random.split(jax.random.key(seed), 8 + 3 * len(NAMES))
    kx, kdy, ka, kb = (jax.random.fold_in(k, part) for k in (kx, kdy, ka, kb))
    kw, km, kv = (keys[i::3] for i in range(3))
    shape = (SEQUENCES, TOKENS, D)
    much_x, much_dy = jax.random.uniform(kz, (2,), jnp.float32, 0.0, 1.0)
    loud = 2.0 ** jax.random.uniform(jax.random.fold_in(kz, 1), (), jnp.float32, -1.0, 2.0)
    layers = 2.0 ** jax.random.uniform(kl, (LAYERS, 1, 1), jnp.float32, -1.0, 1.0)
    x = together(ka, jax.random.normal(kx, shape, jnp.float32), much_x) * bump(kf, D, 4.0)
    dy = together(kb, jax.random.normal(kdy, shape, jnp.float32), much_dy)
    drawn = {"x": x.astype(jnp.bfloat16), "dy": (loud * dy * (SEQUENCES * TOKENS) ** -0.5).astype(jnp.bfloat16)}
    for key, name in zip(kw, NAMES, strict=True):
        w = jax.random.normal(key, SHAPES[name], jnp.float32) * SHAPES[name][1] ** -0.5
        drawn[name] = (w * {"w_gate": 1.0, "w_up": bump(kh, FF, 4.0), "w_down": layers}[name]).astype(jnp.bfloat16)
    for key, name in zip(km, NAMES, strict=True):
        drawn[f"m_{name}"] = 0.1 * jax.random.normal(key, SHAPES[name], jnp.float32)
    for key, name in zip(kv, NAMES, strict=True):
        drawn[f"v_{name}"] = jax.random.uniform(key, SHAPES[name], jnp.float32, 0.005, 0.015)
    return drawn


def matmul(a, w):
    return jnp.dot(a, w, preferred_element_type=jnp.float32).astype(jnp.bfloat16)


def normed(h):
    wide = h.astype(jnp.float32)
    scale = lax.rsqrt(jnp.mean(wide**2, -1, keepdims=True) + 1e-6)
    return (wide * scale).astype(jnp.bfloat16)


def layer(h, w):
    a = normed(h)
    gate = jnp.dot(a, w["w_gate"], preferred_element_type=jnp.float32)
    up = jnp.dot(a, w["w_up"], preferred_element_type=jnp.float32)
    return h + matmul((jax.nn.silu(gate) * up).astype(jnp.bfloat16), w["w_down"])


def adamw(w, m, v, g):
    m = 0.9 * m + 0.1 * g
    v = 0.95 * v + 0.05 * g * g
    step = m * lax.rsqrt(v + 1e-8) + 0.1 * w
    return (w - 0.02 * step).astype(jnp.bfloat16), m, v


def stack(weights, h):
    return lax.scan(lambda h, w: (layer(h, w), None), h, weights)[0]


def reference(x, dy, w_gate, w_up, w_down, m_w_gate, m_w_up, m_w_down, v_w_gate, v_w_up, v_w_down):
    weights = dict(zip(NAMES, (w_gate, w_up, w_down), strict=True))

    def take(so_far, sequence):
        h, by_y = sequence
        _, back = jax.vjp(lambda w: stack(w, h), weights)
        return jax.tree.map(lambda total, term: total + term.astype(jnp.float32), so_far, back(by_y)[0]), None

    none_yet = {name: jnp.zeros(w.shape, jnp.float32) for name, w in weights.items()}
    by_weights, _ = lax.scan(take, none_yet, (x, dy))
    gradients = [by_weights[name].astype(jnp.bfloat16).astype(jnp.float32) for name in NAMES]
    new = [
        adamw(w.astype(jnp.float32), m, v, g)
        for w, m, v, g in zip((w_gate, w_up, w_down), (m_w_gate, m_w_up, m_w_down), (v_w_gate, v_w_up, v_w_down), gradients, strict=True)
    ]
    return tuple(one[which] for which in range(3) for one in new)
```

```python
import functools, math
import jax, jax.numpy as jnp
from jax import lax
from jax.experimental import pallas as pl
from jax.experimental.pallas import tpu as pltpu
from jax.sharding import Mesh, PartitionSpec as P

F32, BF16 = jnp.float32, jnp.bfloat16
ORDERS = (("x", "y"), ("y", "x"))
GROUP = ("x", "y", "core")


def fine_mesh(mesh):
    n = mesh.shape["dp"]
    side = math.isqrt(n // 2)
    return Mesh(mesh.devices.reshape(-1, side, n // 2 // side, 2), ("rep", "x", "y", "core"))


def from_ahead(t, axis, k):
    n = lax.axis_size(axis)
    return lax.ppermute(t, axis, [((i + k) % n, i) for i in range(n)])


def block(t, i, dim):
    return lax.dynamic_index_in_dim(t, i, dim, keepdims=False)


def ahead(axis, k):
    n = lax.axis_size(axis)
    return lax.rem(lax.axis_index(axis) + k, n)


def sums(parts):
    return functools.reduce(lambda a, b: a + b, [p.astype(F32) for p in parts])


def exchange(g, order):
    first, second = order
    dim = 0 if first == "x" else 1
    n, n2 = lax.axis_size(first), lax.axis_size(second)
    g = g.reshape(*(lax.axis_size(a) for a in ("x", "y", "core")), -1, g.shape[-1])
    (other,) = yield [(block(g, ahead("core", 1), 2), "core", 1)], 1
    mine = block(g, lax.axis_index("core"), 2)
    of = [sums((block(mine, ahead(first, k), dim), block(other, ahead(first, k), dim))) for k in range(n)]
    came = yield [(of[k].astype(BF16), first, n - k) for k in range(1, n)], 2
    of = [sums([block(of[0], ahead(second, k), 0)] + [block(c, ahead(second, k), 0) for c in came]) for k in range(n2)]
    came = yield [(of[k].astype(BF16), second, n2 - k) for k in range(1, n2)], 1
    return sums([of[0]] + came)


class Traffic:
    def __init__(self):
        self.flying = []

    def go_on(self, flight, came):
        try:
            flight["sends"], flight["slots"] = next(flight["way"]) if came is None else flight["way"].send(came)
        except StopIteration as end:
            flight["sends"] = None
            flight["done"](end.value)

    def between(self, out, into, new=()):
        for f in self.flying:
            f["slots"] -= 1
        due = [f for f in self.flying if f["slots"] <= 0]
        came, out, into = lax.optimization_barrier(([f["came"] for f in due], out, into))
        for f, c in zip(due, came, strict=True):
            self.go_on(f, c)
        if new:
            way, done = new
            f = {"way": way(out), "done": done}
            self.go_on(f, None)
            due = [f, *due]
            self.flying.append(f)
        due = [f for f in due if f["sends"] is not None]
        self.flying = [f for f in self.flying if f["sends"] is not None]
        arrays, into = lax.optimization_barrier(([[t for t, _, _ in f["sends"]] for f in due], into))
        for f, ts in zip(due, arrays, strict=True):
            f["came"] = [from_ahead(t, axis, k) for t, (_, axis, k) in zip(ts, f["sends"], strict=True)]
        return out, into

    def land(self):
        while self.flying:
            for f in self.flying:
                self.go_on(f, f["came"])
            self.flying = [f for f in self.flying if f["sends"] is not None]
            for f in self.flying:
                f["came"] = [from_ahead(*send) for send in f["sends"]]


def gather_kernel(flows, count, *refs):
    given, outs, (sends, recvs, own_sems) = refs[:count], refs[count : 2 * count], refs[2 * count :]
    me = {a: lax.axis_index(a) for a in GROUP}
    side = {a: lax.axis_size(a) for a in GROUP}

    def place(axis, k):
        return lax.rem(me[axis] + k + side[axis], side[axis])

    barrier = pltpu.get_barrier_semaphore()
    friends = [("x", 1), ("x", -1), ("y", 1), ("y", -1), ("core", 1)]
    for axis, k in friends:
        pl.semaphore_signal(barrier, inc=1, device_id={axis: place(axis, k)}, device_id_type=pl.DeviceIdType.MESH)
    pl.semaphore_wait(barrier, len(friends))

    copies = {}

    def send(f, number, src, dst, axis, k):
        copies[f, number] = pltpu.make_async_remote_copy(
            src_ref=src,
            dst_ref=dst,
            send_sem=sends.at[f, number],
            recv_sem=recvs.at[f, number],
            device_id={axis: place(axis, k)},
            device_id_type=pl.DeviceIdType.MESH,
        )
        copies[f, number].start()

    def block(f, k, rows):
        w, layer, (first, second) = flows[f]
        at = {first: place(first, k), second: me[second]}
        return outs[w].at[layer, at["x"], at["y"], me["core"], rows]

    def piece(f, k, which=slice(None)):
        w, layer, (first, second) = flows[f]
        at = {first: which, second: place(second, k)}
        return outs[w].at[layer, at["x"], at["y"], me["core"]]

    every = range(len(flows))
    owns = []
    for f in every:
        w, layer, (first, second) = flows[f]
        mine = given[w].at[layer]
        whole = pl.ds(0, mine.shape[0])
        owns.append(pltpu.make_async_copy(mine, block(f, 0, whole), own_sems.at[f]))
        owns[f].start()
        send(f, 0, mine, block(f, 0, whole), first, 1)
        send(f, 1, mine, block(f, 0, whole), first, -1)
    for f in every:
        w, layer, (first, second) = flows[f]
        rows = given[w].shape[1]
        half = rows // 16 * 8
        low, high = pl.ds(0, half), pl.ds(half, rows - half)
        copies[f, 0].wait_recv()
        send(f, 2, block(f, -1, low), block(f, -1, low), first, 1)
        copies[f, 1].wait_recv()
        send(f, 3, block(f, 1, high), block(f, 1, high), first, -1)
    for f in every:
        w, layer, (first, second) = flows[f]
        copies[f, 2].wait_recv()
        copies[f, 3].wait_recv()
        owns[f].wait()
        send(f, 4, piece(f, 0), piece(f, 0), second, 1)
        send(f, 5, piece(f, 0), piece(f, 0), second, -1)
        send(f, 8, piece(f, 0), piece(f, 0), "core", 1)
    for f in every:
        w, layer, (first, second) = flows[f]
        half = side[first] // 2
        low, high = pl.ds(0, half), pl.ds(half, side[first] - half)
        copies[f, 4].wait_recv()
        send(f, 6, piece(f, -1, low), piece(f, -1, low), second, 1)
        send(f, 9, piece(f, -1), piece(f, -1), "core", 1)
        copies[f, 5].wait_recv()
        send(f, 7, piece(f, 1, high), piece(f, 1, high), second, -1)
        send(f, 10, piece(f, 1), piece(f, 1), "core", 1)
    for f in every:
        copies[f, 6].wait_recv()
        copies[f, 7].wait_recv()
        send(f, 11, piece(f, 2), piece(f, 2), "core", 1)
    for f in every:
        for number in range(8, 12):
            copies[f, number].wait_recv()
        for number in range(12):
            copies[f, number].wait_send()


def gather(blocks, orders):
    layers = blocks[0].shape[0]
    sides = tuple(lax.axis_size(a) for a in GROUP)
    flows = tuple((w, layer, orders[(w + layer) % 2]) for layer in range(layers) for w in range(len(blocks)))
    sent = sum(t.size * 2 for t in blocks)
    outs = pl.pallas_call(
        functools.partial(gather_kernel, flows, len(blocks)),
        out_shape=[jax.ShapeDtypeStruct((layers, *sides, *t.shape[1:]), BF16) for t in blocks],
        in_specs=[pl.BlockSpec(memory_space=pltpu.VMEM)] * len(blocks),
        out_specs=[pl.BlockSpec(memory_space=pl.ANY)] * len(blocks),
        scratch_shapes=[
            pltpu.SemaphoreType.DMA((len(flows), 12)),
            pltpu.SemaphoreType.DMA((len(flows), 12)),
            pltpu.SemaphoreType.DMA((len(flows),)),
        ],
        compiler_params=pltpu.CompilerParams(collective_id=0, has_side_effects=True),
        cost_estimate=pl.CostEstimate(flops=10**9, bytes_accessed=64 * sent, transcendentals=0),
        name="gather",
    )(*blocks)
    return [t.reshape(layers, -1, t.shape[-1]) for t in outs]


def normed(h):
    wide = h.astype(F32)
    scale = lax.rsqrt(jnp.mean(wide**2, -1, keepdims=True) + 1e-6)
    return (wide * scale).astype(BF16)


def dot(a, b, over):
    return lax.dot_general(a, b, (((over[0],), (over[1],)), ((), ())), preferred_element_type=F32).astype(BF16)


def gate_up_kernel(chunk, a, w_gate, w_up, gate, up, act):
    start = pl.program_id(1) * gate.shape[0]
    for m in range(0, gate.shape[0], chunk):
        rows = a[pl.ds(pl.multiple_of(start + m, chunk), chunk), :]
        g = jnp.dot(rows, w_gate[0], preferred_element_type=F32)
        u = jnp.dot(rows, w_up[0], preferred_element_type=F32)
        at = pl.ds(m, chunk)
        gate[at, :] = g
        up[at, :] = u
        act[at, :] = (jax.nn.silu(g) * u).astype(BF16)


def gate_up(a, w_gate, w_up, layer, wide=256, tall=2048, chunk=256):
    tokens, d = a.shape
    ff = w_gate.shape[-1]
    tall = min(tall, tokens)
    weight = pl.BlockSpec((1, d, wide), lambda j, i: (layer, 0, j))
    tile = pl.BlockSpec((tall, wide), lambda j, i: (i, j))
    return pl.pallas_call(
        functools.partial(gate_up_kernel, chunk),
        grid=(ff // wide, tokens // tall),
        in_specs=[pl.BlockSpec((tokens, d), lambda j, i: (0, 0)), weight, weight],
        out_specs=[tile] * 3,
        out_shape=[jax.ShapeDtypeStruct((tokens, ff), t) for t in (F32, F32, BF16)],
        compiler_params=pltpu.CompilerParams(vmem_limit_bytes=56 * 2**20),
        cost_estimate=pl.CostEstimate(
            flops=4 * tokens * d * ff, bytes_accessed=2 * tokens * d + 4 * d * ff + 10 * tokens * ff, transcendentals=tokens * ff
        ),
        name="gate_up",
    )(a, w_gate, w_up)


def back_act_kernel(chunk, dh, w_down, gate, up, dgate, dup):
    start = pl.program_id(1) * gate.shape[0]
    for m in range(0, gate.shape[0], chunk):
        rows = dh[pl.ds(pl.multiple_of(start + m, chunk), chunk), :]
        by_act = lax.dot_general(rows, w_down[0], (((1,), (1,)), ((), ())), preferred_element_type=F32)
        by_act = by_act.astype(BF16).astype(F32)
        at = pl.ds(m, chunk)
        g = gate[at, :]
        s = jax.nn.sigmoid(g)
        gs = g * s
        dup[at, :] = (by_act * gs).astype(BF16)
        dgate[at, :] = (by_act * up[at, :] * (s + gs * (1 - s))).astype(BF16)


def back_act(dh, w_down, gate, up, layer, wide=256, tall=2048, chunk=256):
    tokens, d = dh.shape
    ff = gate.shape[-1]
    tall = min(tall, tokens)
    tile = pl.BlockSpec((tall, wide), lambda j, i: (i, j))
    return pl.pallas_call(
        functools.partial(back_act_kernel, chunk),
        grid=(ff // wide, tokens // tall),
        in_specs=[
            pl.BlockSpec((tokens, d), lambda j, i: (0, 0)),
            pl.BlockSpec((1, wide, d), lambda j, i: (layer, j, 0)),
            tile,
            tile,
        ],
        out_specs=[tile] * 2,
        out_shape=[jax.ShapeDtypeStruct((tokens, ff), BF16)] * 2,
        compiler_params=pltpu.CompilerParams(vmem_limit_bytes=56 * 2**20),
        cost_estimate=pl.CostEstimate(
            flops=2 * tokens * d * ff, bytes_accessed=2 * tokens * d + 2 * d * ff + 12 * tokens * ff, transcendentals=tokens * ff
        ),
        name="back_act",
    )(dh, w_down, gate, up)


def adamw(w, m, v, g):
    m = 0.9 * m + 0.1 * g
    v = 0.95 * v + 0.05 * g * g
    step = m * lax.rsqrt(v + 1e-8) + 0.1 * w
    return (w - 0.02 * step).astype(BF16), m, v


def step(x, dy, *arrays):
    weights, m, v = (arrays[i : i + 3] for i in (0, 3, 6))
    w_gate, w_up, w_down = weights
    layers = w_gate.shape[0]
    h, dh = x[0], dy[0]
    new = [[None] * layers for _ in weights]
    saved = []
    for l in range(layers):
        a = normed(h)
        gate, up, act = gate_up(a, w_gate, w_up, l)
        saved.append((h, a, gate, up, act))
        if l + 1 < layers:
            h = h + dot(act, w_down[l], (1, 0))

    me = (lax.axis_index("x") * lax.axis_size("y") + lax.axis_index("y")) * 2 + lax.axis_index("core")

    traffic = Traffic()

    def update(which, l, of):
        def adopt(g):
            g = g.astype(BF16).astype(F32)
            w = lax.dynamic_slice(weights[which], (l, me * g.shape[0], 0), (1, *g.shape))[0]
            new[which][l] = adamw(w.astype(F32), m[which][l], v[which][l], g)

        if l:
            adopt(lax.psum_scatter(of, GROUP, scatter_dimension=0, tiled=True))
            return ()
        return lambda g: exchange(g, ORDERS[which % 2]), adopt

    for l in reversed(range(layers)):
        h, a, gate, up, act = saved[l]
        by_down = dot(act, dh, (0, 0))
        _, dh = traffic.between(by_down, dh, update(2, l, by_down))
        (dgate, dup), a = traffic.between(back_act(dh, w_down, gate, up, l), a)
        by_gate = dot(a, dgate, (0, 0))
        _, (a, dup) = traffic.between(by_gate, (a, dup), update(0, l, by_gate))
        by_up = dot(a, dup, (0, 0))
        if l:
            _, (dgate, dup) = traffic.between(by_up, (dgate, dup), update(1, l, by_up))
            by_a, dup = traffic.between(dot(dgate, w_gate[l], (1, 1)), dup)
            by_a = by_a + dot(dup, w_up[l], (1, 1))
            dh = dh + jax.vjp(normed, h)[1](by_a)[0]
            _, dh = traffic.between(dh, dh)
        else:
            traffic.between(by_up, (), update(1, l, by_up))
    traffic.land()

    w, m, v = ([jnp.stack([one[k] for one in of]) for of in new] for k in range(3))
    return (*gather(w, ORDERS), *m, *v)


def solution(mesh):
    data, share, whole, theirs = P(("rep", *GROUP)), P(None, GROUP), P(), P("rep", GROUP)
    return jax.shard_map(
        step,
        mesh=fine_mesh(mesh),
        in_specs=(data,) * 2 + (whole,) * 3 + (share,) * 6,
        out_specs=(P("rep"),) * 3 + (theirs,) * 6,
        check_vma=False,
    )
```

```python
import functools, math
import jax, jax.numpy as jnp
from jax import lax
from jax.experimental import pallas as pl
from jax.experimental.pallas import tpu as pltpu
from jax.sharding import Mesh, PartitionSpec as P

F32, BF16 = jnp.float32, jnp.bfloat16
ORDERS = (("x", "y"), ("y", "x"))
GROUP = ("x", "y", "core")


def fine_mesh(mesh):
    n = mesh.shape["dp"]
    side = math.isqrt(n // 2)
    return Mesh(mesh.devices.reshape(-1, side, n // 2 // side, 2), ("rep", "x", "y", "core"))


def from_ahead(t, axis, k):
    n = lax.axis_size(axis)
    return lax.ppermute(t, axis, [((i + k) % n, i) for i in range(n)])


def block(t, i, dim):
    return lax.dynamic_index_in_dim(t, i, dim, keepdims=False)


def ahead(axis, k):
    n = lax.axis_size(axis)
    return lax.rem(lax.axis_index(axis) + k, n)


def sums(parts):
    return functools.reduce(lambda a, b: a + b, [p.astype(F32) for p in parts])


def exchange(g, order):
    first, second = order
    dim = 0 if first == "x" else 1
    n, n2 = lax.axis_size(first), lax.axis_size(second)
    g = g.reshape(*(lax.axis_size(a) for a in ("x", "y", "core")), -1, g.shape[-1])
    (other,) = yield [(block(g, ahead("core", 1), 2), "core", 1)], 1
    mine = block(g, lax.axis_index("core"), 2)
    of = [sums((block(mine, ahead(first, k), dim), block(other, ahead(first, k), dim))) for k in range(n)]
    came = yield [(of[k].astype(BF16), first, n - k) for k in range(1, n)], 2
    of = [sums([block(of[0], ahead(second, k), 0)] + [block(c, ahead(second, k), 0) for c in came]) for k in range(n2)]
    came = yield [(of[k].astype(BF16), second, n2 - k) for k in range(1, n2)], 1
    return sums([of[0]] + came)


class Traffic:
    def __init__(self):
        self.flying = []
        self.queue = []
        self.running = None
        self.started = False

    def go_on(self, flight, came):
        try:
            flight["sends"], flight["slots"] = next(flight["way"]) if came is None else flight["way"].send(came)
        except StopIteration as end:
            flight["sends"] = None
            flight["done"](end.value)

    def between(self, out, into, new=()):
        for f in self.flying:
            f["slots"] -= 1
        due = [f for f in self.flying if f["slots"] <= 0]
        summed = None
        if self.running:
            self.running["slots"] -= 1
            if self.running["slots"] <= 0:
                summed = self.running["sum"]
        came, summed, out, into = lax.optimization_barrier(([f["came"] for f in due], summed, out, into))
        if summed is not None:
            self.running["done"](summed)
            self.running = None
        for f, c in zip(due, came, strict=True):
            self.go_on(f, c)
        if new:
            way, done = new
            f = {"way": way(out), "done": done}
            self.go_on(f, None)
            due = [f, *due]
            self.flying.append(f)
        due = [f for f in due if f["sends"] is not None]
        self.flying = [f for f in self.flying if f["sends"] is not None]
        start = self.queue.pop(0) if self.queue and not self.running else (None, None)
        arrays, of, into = lax.optimization_barrier(([[t for t, _, _ in f["sends"]] for f in due], start[0], into))
        if of is not None:
            self.running = {"sum": lax.psum_scatter(of, GROUP, scatter_dimension=0, tiled=True), "done": start[1]}
            self.running["slots"] = 3 if self.started else 4
            self.started = True
        for f, ts in zip(due, arrays, strict=True):
            f["came"] = [from_ahead(t, axis, k) for t, (_, axis, k) in zip(ts, f["sends"], strict=True)]
        return out, into

    def finish(self):
        if self.running:
            self.running["done"](self.running["sum"])
        for of, done in self.queue:
            done(lax.psum_scatter(of, GROUP, scatter_dimension=0, tiled=True))

    def land(self):
        while self.flying:
            for f in self.flying:
                self.go_on(f, f["came"])
            self.flying = [f for f in self.flying if f["sends"] is not None]
            for f in self.flying:
                f["came"] = [from_ahead(*send) for send in f["sends"]]


def gather_kernel(flows, count, *refs):
    given, outs, (sends, recvs, own_sems) = refs[:count], refs[count : 2 * count], refs[2 * count :]
    me = {a: lax.axis_index(a) for a in GROUP}
    side = {a: lax.axis_size(a) for a in GROUP}

    def place(axis, k):
        return lax.rem(me[axis] + k + side[axis], side[axis])

    barrier = pltpu.get_barrier_semaphore()
    friends = [("x", 1), ("x", -1), ("y", 1), ("y", -1), ("core", 1)]
    for axis, k in friends:
        pl.semaphore_signal(barrier, inc=1, device_id={axis: place(axis, k)}, device_id_type=pl.DeviceIdType.MESH)
    pl.semaphore_wait(barrier, len(friends))

    copies = {}

    def send(f, number, src, dst, axis, k):
        copies[f, number] = pltpu.make_async_remote_copy(
            src_ref=src,
            dst_ref=dst,
            send_sem=sends.at[f, number],
            recv_sem=recvs.at[f, number],
            device_id={axis: place(axis, k)},
            device_id_type=pl.DeviceIdType.MESH,
        )
        copies[f, number].start()

    def block(f, k, rows):
        w, layer, (first, second) = flows[f]
        at = {first: place(first, k), second: me[second]}
        return outs[w].at[layer, at["x"], at["y"], me["core"], rows]

    def piece(f, k, which=slice(None)):
        w, layer, (first, second) = flows[f]
        at = {first: which, second: place(second, k)}
        return outs[w].at[layer, at["x"], at["y"], me["core"]]

    every = range(len(flows))
    owns = []
    for f in every:
        w, layer, (first, second) = flows[f]
        mine = given[w].at[layer]
        whole = pl.ds(0, mine.shape[0])
        owns.append(pltpu.make_async_copy(mine, block(f, 0, whole), own_sems.at[f]))
        owns[f].start()
        send(f, 0, mine, block(f, 0, whole), first, 1)
        send(f, 1, mine, block(f, 0, whole), first, -1)
    for f in every:
        w, layer, (first, second) = flows[f]
        rows = given[w].shape[1]
        half = rows // 16 * 8
        low, high = pl.ds(0, half), pl.ds(half, rows - half)
        copies[f, 0].wait_recv()
        send(f, 2, block(f, -1, low), block(f, -1, low), first, 1)
        copies[f, 1].wait_recv()
        send(f, 3, block(f, 1, high), block(f, 1, high), first, -1)
    for f in every:
        w, layer, (first, second) = flows[f]
        copies[f, 2].wait_recv()
        copies[f, 3].wait_recv()
        owns[f].wait()
        send(f, 4, piece(f, 0), piece(f, 0), second, 1)
        send(f, 5, piece(f, 0), piece(f, 0), second, -1)
        send(f, 8, piece(f, 0), piece(f, 0), "core", 1)
    for f in every:
        w, layer, (first, second) = flows[f]
        half = side[first] // 2
        low, high = pl.ds(0, half), pl.ds(half, side[first] - half)
        copies[f, 4].wait_recv()
        send(f, 6, piece(f, -1, low), piece(f, -1, low), second, 1)
        send(f, 9, piece(f, -1), piece(f, -1), "core", 1)
        copies[f, 5].wait_recv()
        send(f, 7, piece(f, 1, high), piece(f, 1, high), second, -1)
        send(f, 10, piece(f, 1), piece(f, 1), "core", 1)
    for f in every:
        copies[f, 6].wait_recv()
        copies[f, 7].wait_recv()
        send(f, 11, piece(f, 2), piece(f, 2), "core", 1)
    for f in every:
        for number in range(8, 12):
            copies[f, number].wait_recv()
        for number in range(12):
            copies[f, number].wait_send()


def gather(blocks, orders):
    layers = blocks[0].shape[0]
    sides = tuple(lax.axis_size(a) for a in GROUP)
    flows = tuple((w, layer, orders[(w + layer) % 2]) for layer in range(layers) for w in range(len(blocks)))
    sent = sum(t.size * 2 for t in blocks)
    outs = pl.pallas_call(
        functools.partial(gather_kernel, flows, len(blocks)),
        out_shape=[jax.ShapeDtypeStruct((layers, *sides, *t.shape[1:]), BF16) for t in blocks],
        in_specs=[pl.BlockSpec(memory_space=pltpu.VMEM)] * len(blocks),
        out_specs=[pl.BlockSpec(memory_space=pl.ANY)] * len(blocks),
        scratch_shapes=[
            pltpu.SemaphoreType.DMA((len(flows), 12)),
            pltpu.SemaphoreType.DMA((len(flows), 12)),
            pltpu.SemaphoreType.DMA((len(flows),)),
        ],
        compiler_params=pltpu.CompilerParams(collective_id=0, has_side_effects=True),
        cost_estimate=pl.CostEstimate(flops=10**9, bytes_accessed=64 * sent, transcendentals=0),
        name="gather",
    )(*blocks)
    return [t.reshape(layers, -1, t.shape[-1]) for t in outs]


def normed(h):
    wide = h.astype(F32)
    scale = lax.rsqrt(jnp.mean(wide**2, -1, keepdims=True) + 1e-6)
    return (wide * scale).astype(BF16)


def dot(a, b, over):
    return lax.dot_general(a, b, (((over[0],), (over[1],)), ((), ())), preferred_element_type=F32).astype(BF16)


def gate_up_kernel(chunk, a, w_gate, w_up, gate, up, act):
    start = pl.program_id(1) * gate.shape[0]
    for m in range(0, gate.shape[0], chunk):
        rows = a[pl.ds(pl.multiple_of(start + m, chunk), chunk), :]
        g = jnp.dot(rows, w_gate[0], preferred_element_type=F32)
        u = jnp.dot(rows, w_up[0], preferred_element_type=F32)
        at = pl.ds(m, chunk)
        gate[at, :] = g
        up[at, :] = u
        act[at, :] = (jax.nn.silu(g) * u).astype(BF16)


def gate_up(a, w_gate, w_up, layer, wide=256, tall=2048, chunk=256):
    tokens, d = a.shape
    ff = w_gate.shape[-1]
    tall = min(tall, tokens)
    weight = pl.BlockSpec((1, d, wide), lambda j, i: (layer, 0, j))
    tile = pl.BlockSpec((tall, wide), lambda j, i: (i, j))
    return pl.pallas_call(
        functools.partial(gate_up_kernel, chunk),
        grid=(ff // wide, tokens // tall),
        in_specs=[pl.BlockSpec((tokens, d), lambda j, i: (0, 0)), weight, weight],
        out_specs=[tile] * 3,
        out_shape=[jax.ShapeDtypeStruct((tokens, ff), t) for t in (F32, F32, BF16)],
        compiler_params=pltpu.CompilerParams(vmem_limit_bytes=56 * 2**20),
        cost_estimate=pl.CostEstimate(
            flops=4 * tokens * d * ff, bytes_accessed=2 * tokens * d + 4 * d * ff + 10 * tokens * ff, transcendentals=tokens * ff
        ),
        name="gate_up",
    )(a, w_gate, w_up)


def back_act_kernel(chunk, dh, w_down, gate, up, dgate, dup):
    start = pl.program_id(1) * gate.shape[0]
    for m in range(0, gate.shape[0], chunk):
        rows = dh[pl.ds(pl.multiple_of(start + m, chunk), chunk), :]
        by_act = lax.dot_general(rows, w_down[0], (((1,), (1,)), ((), ())), preferred_element_type=F32)
        by_act = by_act.astype(BF16).astype(F32)
        at = pl.ds(m, chunk)
        g = gate[at, :]
        s = jax.nn.sigmoid(g)
        gs = g * s
        dup[at, :] = (by_act * gs).astype(BF16)
        dgate[at, :] = (by_act * up[at, :] * (s + gs * (1 - s))).astype(BF16)


def back_act(dh, w_down, gate, up, layer, wide=256, tall=2048, chunk=256):
    tokens, d = dh.shape
    ff = gate.shape[-1]
    tall = min(tall, tokens)
    tile = pl.BlockSpec((tall, wide), lambda j, i: (i, j))
    return pl.pallas_call(
        functools.partial(back_act_kernel, chunk),
        grid=(ff // wide, tokens // tall),
        in_specs=[
            pl.BlockSpec((tokens, d), lambda j, i: (0, 0)),
            pl.BlockSpec((1, wide, d), lambda j, i: (layer, j, 0)),
            tile,
            tile,
        ],
        out_specs=[tile] * 2,
        out_shape=[jax.ShapeDtypeStruct((tokens, ff), BF16)] * 2,
        compiler_params=pltpu.CompilerParams(vmem_limit_bytes=56 * 2**20),
        cost_estimate=pl.CostEstimate(
            flops=2 * tokens * d * ff, bytes_accessed=2 * tokens * d + 2 * d * ff + 12 * tokens * ff, transcendentals=tokens * ff
        ),
        name="back_act",
    )(dh, w_down, gate, up)


def adamw(w, m, v, g):
    m = 0.9 * m + 0.1 * g
    v = 0.95 * v + 0.05 * g * g
    step = m * lax.rsqrt(v + 1e-8) + 0.1 * w
    return (w - 0.02 * step).astype(BF16), m, v


def step(x, dy, *arrays):
    weights, m, v = (arrays[i : i + 3] for i in (0, 3, 6))
    w_gate, w_up, w_down = weights
    layers = w_gate.shape[0]
    h, dh = x[0], dy[0]
    sums_of = [[None] * layers for _ in weights]
    saved = []
    for l in range(layers):
        a = normed(h)
        gate, up, act = gate_up(a, w_gate, w_up, l)
        saved.append((h, a, gate, up, act))
        if l + 1 < layers:
            h = h + dot(act, w_down[l], (1, 0))

    me = (lax.axis_index("x") * lax.axis_size("y") + lax.axis_index("y")) * 2 + lax.axis_index("core")

    traffic = Traffic()

    def update(which, l, of):
        def adopt(g):
            sums_of[which][l] = g.astype(BF16)

        if l:
            traffic.queue.append((of, adopt))
            return ()
        return lambda g: exchange(g, ORDERS[which % 2]), adopt

    for l in reversed(range(layers)):
        h, a, gate, up, act = saved[l]
        by_down = dot(act, dh, (0, 0))
        _, dh = traffic.between(by_down, dh, update(2, l, by_down))
        (dgate, dup), a = traffic.between(back_act(dh, w_down, gate, up, l), a)
        by_gate = dot(a, dgate, (0, 0))
        _, (a, dup) = traffic.between(by_gate, (a, dup), update(0, l, by_gate))
        by_up = dot(a, dup, (0, 0))
        if l:
            _, (dgate, dup) = traffic.between(by_up, (dgate, dup), update(1, l, by_up))
            by_a, dup = traffic.between(dot(dgate, w_gate[l], (1, 1)), dup)
            by_a = by_a + dot(dup, w_up[l], (1, 1))
            dh = dh + jax.vjp(normed, h)[1](by_a)[0]
            _, dh = traffic.between(dh, dh)
        else:
            traffic.between(by_up, (), update(1, l, by_up))
    traffic.finish()
    traffic.land()

    new = []
    for which, of in enumerate(sums_of):
        g = jnp.stack(of)
        w = lax.dynamic_slice_in_dim(weights[which], me * g.shape[1], g.shape[1], 1)
        new.append(adamw(w.astype(F32), m[which], v[which], g.astype(F32)))
    w, m, v = zip(*new, strict=True)
    return (*gather(w, ORDERS), *m, *v)


def solution(mesh):
    data, share, whole, theirs = P(("rep", *GROUP)), P(None, GROUP), P(), P("rep", GROUP)
    return jax.shard_map(
        step,
        mesh=fine_mesh(mesh),
        in_specs=(data,) * 2 + (whole,) * 3 + (share,) * 6,
        out_specs=(P("rep"),) * 3 + (theirs,) * 6,
        check_vma=False,
    )
```
